32 devices in a mesh: rep: 4 (over x, y), dp: 8 (over z, core).
Axes of the slice: x: 2, y: 2, z: 4, core: 2. Of those that a mesh axis runs over, the one named last changes fastest.
Arguments:
- x: bfloat16 [32, 2048, 512], P(('rep', 'dp')), parts along dimension 0
- dy: bfloat16 [32, 2048, 512], P(('rep', 'dp')), parts along dimension 0
- wq: bfloat16 [2, 512, 512], replicated
- wk: bfloat16 [2, 512, 512], replicated
- wv: bfloat16 [2, 512, 512], replicated
- wo: bfloat16 [2, 512, 512], replicated
- w_gate: bfloat16 [2, 512, 2048], replicated
- w_up: bfloat16 [2, 512, 2048], replicated
- w_down: bfloat16 [2, 2048, 512], replicated
- m_wq: float32 [2, 512, 512], P(None, 'dp')
- m_wk: float32 [2, 512, 512], P(None, 'dp')
- m_wv: float32 [2, 512, 512], P(None, 'dp')
- m_wo: float32 [2, 512, 512], P(None, 'dp')
- m_w_gate: float32 [2, 512, 2048], P(None, 'dp')
- m_w_up: float32 [2, 512, 2048], P(None, 'dp')
- m_w_down: float32 [2, 2048, 512], P(None, 'dp')
- v_wq: float32 [2, 512, 512], P(None, 'dp')
- v_wk: float32 [2, 512, 512], P(None, 'dp')
- v_wv: float32 [2, 512, 512], P(None, 'dp')
- v_wo: float32 [2, 512, 512], P(None, 'dp')
- v_w_gate: float32 [2, 512, 2048], P(None, 'dp')
- v_w_up: float32 [2, 512, 2048], P(None, 'dp')
- v_w_down: float32 [2, 2048, 512], P(None, 'dp')
Outputs:
- output 1: bfloat16 [8, 512, 512], P('rep'), parts along dimension 0
- output 2: bfloat16 [8, 512, 512], P('rep'), parts along dimension 0
- output 3: bfloat16 [8, 512, 512], P('rep'), parts along dimension 0
- output 4: bfloat16 [8, 512, 512], P('rep'), parts along dimension 0
- output 5: bfloat16 [8, 512, 2048], P('rep'), parts along dimension 0
- output 6: bfloat16 [8, 512, 2048], P('rep'), parts along dimension 0
- output 7: bfloat16 [8, 2048, 512], P('rep'), parts along dimension 0
- output 8: float32 [8, 512, 512], P('rep', 'dp'), parts along dimension 0
- output 9: float32 [8, 512, 512], P('rep', 'dp'), parts along dimension 0
- output 10: float32 [8, 512, 512], P('rep', 'dp'), parts along dimension 0
- output 11: float32 [8, 512, 512], P('rep', 'dp'), parts along dimension 0
- output 12: float32 [8, 512, 2048], P('rep', 'dp'), parts along dimension 0
- output 13: float32 [8, 512, 2048], P('rep', 'dp'), parts along dimension 0
- output 14: float32 [8, 2048, 512], P('rep', 'dp'), parts along dimension 0
- output 15: float32 [8, 512, 512], P('rep', 'dp'), parts along dimension 0
- output 16: float32 [8, 512, 512], P('rep', 'dp'), parts along dimension 0
- output 17: float32 [8, 512, 512], P('rep', 'dp'), parts along dimension 0
- output 18: float32 [8, 512, 512], P('rep', 'dp'), parts along dimension 0
- output 19: float32 [8, 512, 2048], P('rep', 'dp'), parts along dimension 0
- output 20: float32 [8, 512, 2048], P('rep', 'dp'), parts along dimension 0
- output 21: float32 [8, 2048, 512], P('rep', 'dp'), parts along dimension 0
There are 4 independent parts. The reference program is written for one: setup_inputs(seed, part) draws one part's arguments, and reference() takes and returns one part's arrays. A program takes and returns all parts, laid end to end along the dimension named above; an argument that names none is the same for every part.
All inputs are finite; a program needn't handle non-finite values.
Results may differ from the reference program's by a relative error of at most 0.024.
Values are sent between devices in bfloat16 or wider.
A program may use at most 2 GiB of HBM per device.

```python
import jax
import jax.numpy as jnp
from jax import lax

SEQUENCES = 8
TOKENS = 2048
D = 512
HEADS = 4
KV_HEADS = 4
HEAD = 128
FF = 2048
LAYERS = 2
THETA = 10000
NAMES = ("wq", "wk", "wv", "wo", "w_gate", "w_up", "w_down")
SHAPES = {
    "wq": (LAYERS, D, HEADS * HEAD),
    "wk": (LAYERS, D, KV_HEADS * HEAD),
    "wv": (LAYERS, D, KV_HEADS * HEAD),
    "wo": (LAYERS, HEADS * HEAD, D),
    "w_gate": (LAYERS, D, FF),
    "w_up": (LAYERS, D, FF),
    "w_down": (LAYERS, FF, D),
}


def bump(key, n, height):
    away = (jnp.arange(n, dtype=jnp.int32) - jax.random.randint(key, (), 0, n, jnp.int32)) % n
    return jnp.where(away < n // 8, height, 1.0)


def together(key, own, strength):
    shared = jax.random.normal(key, own.shape[1:], jnp.float32)
    return (own + strength * shared) * lax.rsqrt(1 + strength * strength)


def setup_inputs(seed: int = 0, part: int = 0) -> dict:
    kx, kdy, ka, kb, kz, kf, kh, kl, *keys = jax.random.split(jax.random.key(seed), 8 + 3 * len(NAMES))
    kx, kdy, ka, kb = (jax.random.fold_in(k, part) for k in (kx, kdy, ka, kb))
    kw, km, kv = (keys[i::3] for i in range(3))
    shape = (SEQUENCES, TOKENS, D)
    much_x, much_dy = jax.random.uniform(kz, (2,), jnp.float32, 0.0, 1.0)
    loud = 2.0 ** jax.random.uniform(jax.random.fold_in(kz, 1), (), jnp.float32, -1.0, 2.0)
    layers = 2.0 ** jax.random.uniform(kl, (LAYERS, 1, 1), jnp.float32, -1.0, 1.0)
    times = {"wq": 1.0, "wk": 1.0, "wv": 2.0, "wo": layers, "w_gate": 1.0, "w_up": bump(kh, FF, 4.0), "w_down": layers}
    x = together(ka, jax.random.normal(kx, shape, jnp.float32), much_x) * bump(kf, D, 4.0)
    dy = together(kb, jax.random.normal(kdy, shape, jnp.float32), much_dy)
    drawn = {"x": x.astype(jnp.bfloat16), "dy": (loud * dy * (SEQUENCES * TOKENS) ** -0.5).astype(jnp.bfloat16)}
    for key, name in zip(kw, NAMES, strict=True):
        drawn[name] = (jax.random.normal(key, SHAPES[name], jnp.float32) * SHAPES[name][1] ** -0.5 * times[name]).astype(jnp.bfloat16)
    for key, name in zip(km, NAMES, strict=True):
        drawn[f"m_{name}"] = 0.1 * jax.random.normal(key, SHAPES[name], jnp.float32)
    for key, name in zip(kv, NAMES, strict=True):
        drawn[f"v_{name}"] = loud * loud * jax.random.uniform(key, SHAPES[name], jnp.float32, 0.2, 0.6)
    return drawn


def matmul(a, w):
    return jnp.dot(a, w, preferred_element_type=jnp.float32).astype(jnp.bfloat16)


def normed(h):
    wide = h.astype(jnp.float32)
    scale = lax.rsqrt(jnp.mean(wide**2, -1, keepdims=True) + 1e-6)
    return (wide * scale).astype(jnp.bfloat16)


def turned(t, theta):
    half = t.shape[-1] // 2
    angle = jnp.arange(t.shape[0], dtype=jnp.float32)[:, None] * theta ** (-jnp.arange(half, dtype=jnp.float32) / half)
    cos, sin = jnp.cos(angle)[:, None], jnp.sin(angle)[:, None]
    a, b = t[..., :half].astype(jnp.float32), t[..., half:].astype(jnp.float32)
    return jnp.concatenate([a * cos - b * sin, b * cos + a * sin], -1).astype(jnp.bfloat16)


def seen_by(q, k, v):
    tokens, kv = q.shape[0], k.shape[1]
    q = q.reshape(tokens, kv, -1, q.shape[-1])
    scores = jnp.einsum("tgsd,ugd->gstu", q.astype(jnp.float32), k.astype(jnp.float32)) * q.shape[-1] ** -0.5
    place = jnp.arange(tokens)
    weights = jax.nn.softmax(jnp.where(place[:, None] >= place, scores, -jnp.inf), -1).astype(jnp.bfloat16)
    return jnp.einsum("gstu,ugd->tgsd", weights.astype(jnp.float32), v.astype(jnp.float32)).astype(jnp.bfloat16).reshape(tokens, -1)


def layer(h, w):
    a = normed(h)
    q, k = (turned(matmul(a, w[name]).reshape(h.shape[0], -1, HEAD), THETA) for name in ("wq", "wk"))
    h = h + matmul(seen_by(q, k, matmul(a, w["wv"]).reshape(h.shape[0], -1, HEAD)), w["wo"])
    b = normed(h)
    gate = jnp.dot(b, w["w_gate"], preferred_element_type=jnp.float32)
    up = jnp.dot(b, w["w_up"], preferred_element_type=jnp.float32)
    return h + matmul((jax.nn.silu(gate) * up).astype(jnp.bfloat16), w["w_down"])


def adamw(w, m, v, g):
    m = 0.9 * m + 0.1 * g
    v = 0.95 * v + 0.05 * g * g
    step = m * lax.rsqrt(v + 1e-8) + 0.1 * w
    return (w - 0.02 * step).astype(jnp.bfloat16), m, v


def stack(weights, h):
    return lax.scan(lambda h, w: (layer(h, w), None), h, weights)[0]


def reference(x, dy, wq, wk, wv, wo, w_gate, w_up, w_down, m_wq, m_wk, m_wv, m_wo, m_w_gate, m_w_up, m_w_down, v_wq, v_wk, v_wv, v_wo, v_w_gate, v_w_up, v_w_down):
    weights = dict(zip(NAMES, (wq, wk, wv, wo, w_gate, w_up, w_down), strict=True))

    def take(so_far, sequence):
        h, by_y = sequence
        _, back = jax.vjp(stack, weights, h)
        by_weights, by_h = back(by_y)
        return jax.tree.map(lambda total, term: total + term.astype(jnp.float32), so_far, by_weights), by_h

    none_yet = {name: jnp.zeros(w.shape, jnp.float32) for name, w in weights.items()}
    by_weights, by_x = lax.scan(take, none_yet, (x, dy))
    gradients = [by_weights[name].astype(jnp.bfloat16).astype(jnp.float32) for name in NAMES]
    first = (m_wq, m_wk, m_wv, m_wo, m_w_gate, m_w_up, m_w_down)
    second = (v_wq, v_wk, v_wv, v_wo, v_w_gate, v_w_up, v_w_down)
    new = [adamw(weights[name].astype(jnp.float32), m, v, g) for name, m, v, g in zip(NAMES, first, second, gradients, strict=True)]
    return tuple(one[which] for which in range(3) for one in new)
```

```python
import numpy as np

import jax
import jax.numpy as jnp
from jax import lax
from jax.experimental import pallas as pl
from jax.experimental.pallas import tpu as pltpu
from jax.sharding import PartitionSpec as P

NEG = -1e30
LOG2E = 1.4426950408889634
HEAD = 128
THETA = 10000
BF, F32 = jnp.bfloat16, jnp.float32
ROWS = 512
PART = 512
LOCAL, REMOTE = 60 * 2**20, 28 * 2**20
MESH = pl.DeviceIdType.MESH


def _dot(a, b, ca, cb):
    return lax.dot_general(a, b, (((ca,), (cb,)), ((), ())), preferred_element_type=F32)


def _table(tokens):
    half = HEAD // 2
    angle = np.arange(tokens, dtype=np.float32)[:, None] * np.float32(THETA) ** (-np.arange(half, dtype=np.float32) / np.float32(half))
    return np.concatenate([np.cos(angle), np.sin(angle)], -1).astype(np.float32)


def _angles(tab):
    other = pltpu.roll(tab, HEAD // 2, 1)
    first = lax.broadcasted_iota(jnp.int32, tab.shape, 1) < HEAD // 2
    return jnp.where(first, tab, other), jnp.where(first, -other, tab)


def _normed(h):
    wide = h.astype(F32)
    scale = lax.rsqrt(jnp.mean(wide * wide, -1, keepdims=True) + 1e-6)
    return wide, scale, (wide * scale).astype(BF)


def _norm_back(wide, scale, d):
    dot = jnp.mean(d * wide, -1, keepdims=True)
    return scale * d - wide * (scale * scale * scale * dot)


def _heads(ref):
    return jnp.concatenate([ref[n] for n in range(ref.shape[0])], axis=1)


def _call(body, grid, given, ins, outs, out_specs, scratch=(), flops=0, aliases=None, prefetch=0, room=LOCAL):
    return pl.pallas_call(
        body,
        grid_spec=pltpu.PrefetchScalarGridSpec(num_scalar_prefetch=prefetch, grid=grid, in_specs=ins, out_specs=out_specs, scratch_shapes=list(scratch)),
        out_shape=outs,
        input_output_aliases=aliases or {},
        compiler_params=pltpu.CompilerParams(dimension_semantics=("arbitrary",) * len(grid), vmem_limit_bytes=room),
        cost_estimate=pl.CostEstimate(flops=flops, transcendentals=0, bytes_accessed=sum(a.size * a.dtype.itemsize for a in [*given, *outs])),
    )(*given)


def _of(shape, dtype=BF):
    return jax.ShapeDtypeStruct(shape, dtype)


def _whole(shape, layer):
    return pl.BlockSpec((None, *shape[1:]), lambda i: (layer, 0, 0), pipeline_mode=pl.Buffered(1))


ROW = lambda d, rows=ROWS: pl.BlockSpec((rows, d), lambda i: (i, 0))
HROW = lambda heads, rows=ROWS: pl.BlockSpec((heads, rows, HEAD), lambda i: (0, i, 0))


def _seen():
    return lax.broadcasted_iota(jnp.int32, (ROWS, ROWS), 1) >= lax.broadcasted_iota(jnp.int32, (ROWS, ROWS), 0)


def _attention_call(body, given, ins, outs, out_specs, scratch, width):
    heads, tokens, _ = given[0].shape
    return _call(body, (tokens // ROWS,), given, ins, outs, out_specs, scratch, flops=heads * tokens * tokens * width)


WHOLE = lambda t: pl.BlockSpec(t.shape, lambda i, *_: (0, 0, 0))
STAT = lambda heads: pl.BlockSpec((heads, ROWS), lambda i, *_: (0, i))


def attend(q, k, v):
    heads, tokens, d = q.shape
    scale = d**-0.5
    e = scale * LOG2E

    def body(q_ref, k_ref, v_ref, o_ref, lse_ref, top_s, mix_s):
        iq = pl.program_id(0)
        top_s[...] = jnp.full(top_s.shape, NEG, F32)
        mix_s[...] = jnp.zeros_like(mix_s)
        ones = jnp.ones((8, ROWS), BF)

        def block(j, ok):
            here = pl.ds(j * ROWS, ROWS)
            scores = [_dot(k_ref[n, here, :], q_ref[n], 1, 1) for n in range(heads)]
            weights, keeps = [], []
            for n, s in enumerate(scores):
                if ok is not None:
                    s = jnp.where(ok, s, 2 * NEG)
                old = top_s[n : n + 1, :]
                top = jnp.maximum(old, s.max(axis=0, keepdims=True))
                top_s[n : n + 1, :] = top
                weights.append(jnp.exp2((s - top) * e).astype(BF))
                keeps.append(jnp.exp2((old - top) * e))
            for n, (p, keep) in enumerate(zip(weights, keeps)):
                values = jnp.concatenate([v_ref[n, here, :].T, ones], axis=0)
                mix_s[n] = mix_s[n] * keep + _dot(values, p, 1, 0)

        lax.fori_loop(0, iq, lambda j, _: block(j, None), None)
        block(iq, _seen())
        for n in range(heads):
            total = mix_s[n, d : d + 1, :]
            o_ref[n] = (mix_s[n, :d, :] * (1 / total)).T.astype(BF)
            lse_ref[n : n + 1, :] = top_s[n : n + 1, :] * scale + jnp.log(total)

    return _attention_call(body, [q, k, v], [HROW(heads), WHOLE(k), WHOLE(v)], [_of(q.shape), _of((heads, tokens), F32)],
                           [HROW(heads), STAT(heads)], [pltpu.VMEM((heads, ROWS), F32), pltpu.VMEM((heads, d + 8, ROWS), F32)], 2 * d)


def attend_back(q, k, v, do, lse, delta):
    heads, tokens, d = q.shape
    scale = d**-0.5
    e = scale * LOG2E

    def body(q_ref, k_ref, v_ref, do_ref, lse_ref, delta_ref, dq_ref, dk_ref, dv_ref, dq_s, dk_s, dv_s):
        iq = pl.program_id(0)

        @pl.when(iq == 0)
        def _():
            dk_s[...] = jnp.zeros_like(dk_s)
            dv_s[...] = jnp.zeros_like(dv_s)

        dq_s[...] = jnp.zeros_like(dq_s)

        def block(j, ok):
            here = pl.ds(j * ROWS, ROWS)
            scores = [_dot(k_ref[n, here, :], q_ref[n], 1, 1) for n in range(heads)]
            dps = [_dot(v_ref[n, here, :], do_ref[n], 1, 1) for n in range(heads)]
            for n in range(heads):
                p = jnp.exp2(scores[n] * e - lse_ref[n : n + 1, :] * LOG2E)
                if ok is not None:
                    p = jnp.where(ok, p, 0.0)
                ds = (p * (dps[n] - delta_ref[n : n + 1, :])).astype(BF)
                dv_s[n, here, :] += _dot(p.astype(BF), do_ref[n], 1, 0)
                dk_s[n, here, :] += _dot(ds, q_ref[n], 1, 0)
                dq_s[n] += _dot(k_ref[n, here, :].T, ds, 1, 0)

        lax.fori_loop(0, iq, lambda j, _: block(j, None), None)
        block(iq, _seen())
        for n in range(heads):
            dq_ref[n] = (dq_s[n] * scale).T.astype(BF)

        @pl.when(iq == pl.num_programs(0) - 1)
        def _():
            dk_ref[...] = (dk_s[...] * scale).astype(BF)
            dv_ref[...] = dv_s[...].astype(BF)

    return _attention_call(body, [q, k, v, do, lse, delta], [HROW(heads), WHOLE(k), WHOLE(v), HROW(heads), STAT(heads), STAT(heads)], [_of(q.shape)] * 3,
                           [HROW(heads), WHOLE(k), WHOLE(v)], [pltpu.VMEM((heads, d, ROWS), F32)] + [pltpu.VMEM(k.shape, F32)] * 2, 5 * d)


def project(h, table, wq, wk, wv, layer):
    tokens, d = h.shape
    heads = wq.shape[2] // HEAD

    def body(h_ref, tab_ref, wq_ref, wk_ref, wv_ref, q_ref, k_ref, v_ref):
        a = _normed(h_ref[...])[2]
        cos, sin = _angles(tab_ref[...])
        for w_ref, o_ref, turn in ((wq_ref, q_ref, True), (wk_ref, k_ref, True), (wv_ref, v_ref, False)):
            t = _dot(a, w_ref[...], 1, 0).astype(BF)
            for n in range(heads):
                x = t[:, n * HEAD : (n + 1) * HEAD]
                if turn:
                    x = x.astype(F32)
                    x = (x * cos + pltpu.roll(x, HEAD // 2, 1) * sin).astype(BF)
                o_ref[n] = x

    given = [h, table, wq, wk, wv]
    return _call(body, (tokens // ROWS,), given, [ROW(d), ROW(HEAD)] + [_whole(wq.shape, layer)] * 3, [_of((heads, tokens, HEAD))] * 3,
                 [HROW(heads)] * 3, flops=2 * tokens * d * d * 3)


def feed(h, o, wo, wg, wu, wd, layer):
    tokens, d = h.shape
    heads, ff = o.shape[0], wg.shape[2]

    def body(h_ref, o_ref, wo_ref, wg_ref, wu_ref, wd_ref, out_ref):
        mid = (h_ref[...].astype(F32) + _dot(_heads(o_ref), wo_ref[...], 1, 0).astype(BF).astype(F32)).astype(BF)
        b = _normed(mid)[2]
        down = jnp.zeros((ROWS, d), F32)
        for at in range(0, ff, PART):
            gate = _dot(b, wg_ref[:, at : at + PART], 1, 0)
            up = _dot(b, wu_ref[:, at : at + PART], 1, 0)
            act = (gate * lax.logistic(gate) * up).astype(BF)
            down += _dot(act, wd_ref[at : at + PART, :], 1, 0)
        out_ref[...] = (mid.astype(F32) + down.astype(BF).astype(F32)).astype(BF)

    given = [h, o, wo, wg, wu, wd]
    return _call(body, (tokens // ROWS,), given, [ROW(d), HROW(heads)] + [_whole(w.shape, layer) for w in (wo, wg, wu, wd)], [_of((tokens, d))],
                 [ROW(d)], flops=2 * tokens * d * (d + 3 * ff))[0]


def feed_back(h, o, dh, wo, wg, wu, wd, layer, devices):
    tokens, d = h.shape
    heads, ff = o.shape[0], wg.shape[2]
    tall_width, wide_width = ff + d, 3 * d + 2 * ff
    mine, tall = d // devices, ff // devices
    fold = tall // mine

    def body(h_ref, o_ref, dh_ref, wo_ref, wg_ref, wu_ref, wd_ref, dmid_ref, do_ref, delta_ref, tall_ref, wide_ref, ag, au, ad, ao):
        i = pl.program_id(0)

        @pl.when(i == 0)
        def _():
            for ref in (ag, au, ad, ao):
                ref[...] = jnp.zeros_like(ref)

        o = _heads(o_ref)
        mid = (h_ref[...].astype(F32) + _dot(o, wo_ref[...], 1, 0).astype(BF).astype(F32)).astype(BF)
        wide, scale, b = _normed(mid)
        dy = dh_ref[...]
        bt, dyt = b.T, dy.T
        db = jnp.zeros((ROWS, d), F32)
        for at in range(0, ff, PART):
            here = slice(at, at + PART)
            gate = _dot(b, wg_ref[:, here], 1, 0)
            up = _dot(b, wu_ref[:, here], 1, 0)
            da = _dot(dy, wd_ref[here, :], 1, 1).astype(BF).astype(F32)
            sig = lax.logistic(gate)
            silu = gate * sig
            act = (silu * up).astype(BF)
            dup = (da * silu).astype(BF)
            dgate = (da * up * (sig + silu * (1 - sig))).astype(BF)
            ad[:, here] += _dot(dyt, act, 1, 0)
            au[:, here] += _dot(bt, dup, 1, 0)
            ag[:, here] += _dot(bt, dgate, 1, 0)
            db += _dot(dgate, wg_ref[:, here], 1, 1) + _dot(dup, wu_ref[:, here], 1, 1)
        dmid = (dy.astype(F32) + _norm_back(wide, scale, db.astype(BF).astype(F32)).astype(BF).astype(F32)).astype(BF)
        dmid_ref[...] = dmid
        do = _dot(dmid, wo_ref[...], 1, 1).astype(BF)
        ao[...] += _dot(o.T, dmid, 1, 0)
        for n in range(heads):
            at = slice(n * HEAD, (n + 1) * HEAD)
            do_ref[n] = do[:, at]
            delta_ref[n : n + 1, :] = (do[:, at].astype(F32) * o[:, at].astype(F32)).T.sum(axis=0, keepdims=True)

        @pl.when(i == pl.num_programs(0) - 1)
        def _():
            wide_ref[:, 3 * d : 3 * d + ff] = ag[...].astype(BF)
            wide_ref[:, 3 * d + ff :] = au[...].astype(BF)
            tall_ref[:, ff:] = ao[...].astype(BF)
            for p in range(ff // HEAD):
                t = ad[:, p * HEAD : (p + 1) * HEAD].T.astype(BF)
                for q in range(HEAD // mine):
                    row = p * HEAD + q * mine
                    dev, j = row // tall, row % tall // mine
                    tall_ref[dev * mine : (dev + 1) * mine, j * d : (j + 1) * d] = t[q * mine : (q + 1) * mine, :]

    given = [h, o, dh, wo, wg, wu, wd]
    return _call(
        body, (tokens // ROWS,), given, [ROW(d), HROW(heads), ROW(d)] + [_whole(w.shape, layer) for w in (wo, wg, wu, wd)],
        [_of((tokens, d)), _of((heads, tokens, HEAD)), _of((heads, tokens), F32), _of((d, tall_width)), _of((d, wide_width))],
        [ROW(d), HROW(heads), pl.BlockSpec((heads, ROWS), lambda i: (0, i))]
        + [pl.BlockSpec((d, n), lambda i: (0, 0), pipeline_mode=pl.Buffered(1)) for n in (tall_width, wide_width)],
        [pltpu.VMEM((d, ff), F32)] * 3 + [pltpu.VMEM((d, d), F32)], flops=2 * tokens * d * (8 * ff + 3 * d))


def project_back(g, h, table, dq, dk, dv, dmid, wq, wk, wv, layer):
    tokens, d = h.shape
    heads = dq.shape[0]
    more = dmid is not None

    def body(_, h_ref, tab_ref, dq_ref, dk_ref, dv_ref, *rest):
        i = pl.program_id(0)
        ins, rest = (rest[:4], rest[4:]) if more else ((), rest)
        g_ref, acc = rest[0], rest[-1]
        wide, scale, a = _normed(h_ref[...])
        cos, sin = _angles(tab_ref[...])
        at = a.T

        @pl.when(i == 0)
        def _():
            acc[...] = jnp.zeros_like(acc)

        da = jnp.zeros((ROWS, d), F32)
        for n, (ref, turn) in enumerate(((dq_ref, True), (dk_ref, True), (dv_ref, False))):
            parts = []
            for m in range(heads):
                x = ref[m]
                if turn:
                    x = x.astype(F32)
                    x = (x * cos - pltpu.roll(x, HEAD // 2, 1) * sin).astype(BF)
                parts.append(x)
            t = jnp.concatenate(parts, axis=1)
            acc[:, n * d : (n + 1) * d] += _dot(at, t, 1, 0)
            if more:
                da += _dot(t, ins[1 + n][...], 1, 1)
        if more:
            dh = _norm_back(wide, scale, da.astype(BF).astype(F32)).astype(BF)
            rest[1][...] = (ins[0][...].astype(F32) + dh.astype(F32)).astype(BF)

        @pl.when(i == pl.num_programs(0) - 1)
        def _():
            g_ref[...] = acc[...].astype(BF)

    given = [g, h, table, dq, dk, dv] + ([dmid, wq, wk, wv] if more else [])
    got = _call(
        body, (tokens // ROWS,), given,
        [pl.BlockSpec(memory_space=pl.ANY), ROW(d), ROW(HEAD)] + [HROW(heads)] * 3 + ([ROW(d)] + [_whole(wq.shape, layer)] * 3 if more else []),
        [_of(g.shape)] + ([_of((tokens, d))] if more else []),
        [pl.BlockSpec((d, 3 * d), lambda i: (0, 0), pipeline_mode=pl.Buffered(1))] + ([ROW(d)] if more else []),
        [pltpu.VMEM((d, 3 * d), F32)], flops=2 * tokens * d * d * (6 if more else 3), aliases={0: 0})
    return got[0], got[1] if more else None


def update(me, g, w, m, v, layer, earlier):
    count = len(w)
    rows, width = g.shape
    steps = 4
    small = rows // steps
    folds = [one.shape[1] // rows for one in m]
    view = lambda t, f: t.reshape(t.shape[0], t.shape[1] // rows, rows, t.shape[2])
    given = [me, g] + [view(t, f) for t, f in zip(w, folds)] + [view(t, f) for t, f in zip(m, folds)] + [view(t, f) for t, f in zip(v, folds)]

    def body(me_ref, g_ref, *refs):
        ws, ms, vs = (refs[n * count : (n + 1) * count] for n in range(3))
        outs = refs[-3 * count :]
        at = 0
        for n in range(count):
            cols = ws[n].shape[2]
            for j in range(folds[n]):
                here = slice(at, at + cols)
                g = g_ref[:, here].astype(F32)
                new_m = 0.9 * ms[n][j] + 0.1 * g
                new_v = 0.95 * vs[n][j] + 0.05 * g * g
                old = ws[n][j].astype(F32)
                step = new_m * lax.rsqrt(new_v + 1e-8) + 0.1 * old
                outs[n][j] = (old - 0.02 * step).astype(BF)
                outs[count + n][j] = new_m
                outs[2 * count + n][j] = new_v
                at += cols

    moment = lambda t, f: pl.BlockSpec((None, f, small, t.shape[2]), lambda i, me_ref: (layer, 0, i, 0))
    weight = lambda t, f: pl.BlockSpec((None, f, small, t.shape[2]), lambda i, me_ref: (layer, me_ref[0], i, 0))
    moments = [moment(t, f) for t, f in zip(m, folds)] * 2
    wide = pl.BlockSpec((small, width), lambda i, me_ref: (i, 0))
    ins = [wide] + [weight(t, f) for t, f in zip(w, folds)] + moments
    aliases = {}
    if earlier is not None:
        aliases = {len(given) + n: count + n for n in range(2 * count)}
        given = given + [view(t, f) for t, f in zip(earlier, folds * 2)]
        ins = ins + [pl.BlockSpec(memory_space=pl.ANY)] * (2 * count)
    outs = [_of((f, rows, t.shape[2])) for t, f in zip(m, folds)] + [_of(view(t, f).shape, F32) for t, f in zip(m, folds)] * 2
    blocks = [pl.BlockSpec((f, small, t.shape[2]), lambda i, me_ref: (0, i, 0)) for t, f in zip(m, folds)]
    got = _call(body, (steps,), given, ins, outs, blocks + moments, flops=20 * rows * width, aliases=aliases, prefetch=1, room=REMOTE)
    return [t.reshape(f * rows, t.shape[2]) for t, f in zip(got, folds)], [t.reshape(o.shape) for t, o in zip(got[count:], [*m, *v])]


def gather(blocks, number):
    count, chips = len(blocks), 4

    def body(*refs):
        ins, outs, (up_s, up_r, down_s, down_r, twin_s, twin_r, own_s) = refs[:count], refs[count : 2 * count], refs[2 * count :]
        me = lax.axis_index("dp")
        z, core = me // 2, me % 2
        twin = me + 1 - 2 * core
        above, below = z < chips - 1, z > 0
        barrier = pltpu.get_barrier_semaphore()

        def greet(device):
            pl.semaphore_signal(barrier, inc=1, device_id={"dp": device}, device_id_type=MESH)

        greet(twin)
        pl.when(above)(lambda: greet(me + 2))
        pl.when(below)(lambda: greet(me - 2))
        pl.semaphore_wait(barrier, 1 + above.astype(jnp.int32) + below.astype(jnp.int32))

        def place(n, device):
            rows = ins[n].shape[0]
            return outs[n].at[pl.ds(pl.multiple_of(device * rows, rows), rows), :]

        def copy(n, src, device, sems, k, target):
            return pltpu.make_async_remote_copy(src_ref=src, dst_ref=place(n, device), send_sem=sems[0].at[n, k], recv_sem=sems[1].at[n, k],
                                                device_id={"dp": target}, device_id_type=MESH)

        UPS, DOWNS, TWINS = (up_s, up_r), (down_s, down_r), (twin_s, twin_r)
        each = range(count)
        mine = lambda n: pltpu.make_async_copy(ins[n], place(n, me), own_s.at[n])
        first = lambda n, sems, target: copy(n, ins[n], me, sems, 0, target)
        on = lambda n, device, sems, k, target: copy(n, place(n, device), device, sems, k, target)

        def all_of(what):
            def run():
                for n in each:
                    what(n)

            return run

        pl.when(above)(all_of(lambda n: first(n, UPS, me + 2).start()))
        pl.when(below)(all_of(lambda n: first(n, DOWNS, me - 2).start()))
        for n in each:
            first(n, TWINS, twin).start()
            mine(n).start()
        for t in range(1, chips):
            for near, far, sems, device, target, k in (
                (z >= t, above, UPS, me - 2 * t, me + 2, t), (z + t < chips, below, DOWNS, me + 2 * t, me - 2, chips - 1 + t)):

                @pl.when(near)
                def _():
                    for n in each:
                        on(n, device, sems, t - 1, twin).wait_recv()
                        if t < chips - 1:
                            pl.when(far)(lambda: on(n, device, sems, t, target).start())
                        on(n, device, TWINS, k, twin).start()

        for n in each:
            mine(n).wait()
            first(n, TWINS, twin).wait_send()
            on(n, twin, TWINS, 0, twin).wait_recv()
        pl.when(above)(all_of(lambda n: first(n, UPS, me + 2).wait_send()))
        pl.when(below)(all_of(lambda n: first(n, DOWNS, me - 2).wait_send()))
        for t in range(1, chips):
            for near, far, sems, device, target, k in (
                (z >= t, above, UPS, me - 2 * t, me + 2, t), (z + t < chips, below, DOWNS, me + 2 * t, me - 2, chips - 1 + t)):

                @pl.when(near)
                def _():
                    for n in each:
                        if t < chips - 1:
                            pl.when(far)(lambda: on(n, device, sems, t, target).wait_send())
                        on(n, device, TWINS, k, twin).wait_send()
                        on(n, device + 1 - 2 * core, TWINS, k, twin).wait_recv()

    hops = pltpu.SemaphoreType.DMA((count, chips - 1))
    return pl.pallas_call(
        body,
        in_specs=[pl.BlockSpec(memory_space=pltpu.VMEM)] * count,
        out_specs=[pl.BlockSpec(memory_space=pl.ANY)] * count,
        out_shape=[_of((8 * b.shape[0], b.shape[1])) for b in blocks],
        scratch_shapes=[hops] * 4 + [pltpu.SemaphoreType.DMA((count, 2 * chips - 1))] * 2 + [pltpu.SemaphoreType.DMA((count,))],
        compiler_params=pltpu.CompilerParams(collective_id=number, has_side_effects=True, vmem_limit_bytes=REMOTE),
        cost_estimate=pl.CostEstimate(flops=10**10, transcendentals=0, bytes_accessed=10**7),
    )(*blocks)


def solution(mesh):
    devices = mesh.shape["dp"]

    def step(x, dy, *arrays):
        weights, m, v = (arrays[i : i + 7] for i in (0, 7, 14))
        wq, wk, wv, wo, wg, wu, wd = weights
        table = jnp.asarray(_table(x.shape[1]))
        layers = wq.shape[0]
        me = lax.axis_index("dp").astype(jnp.int32)[None]
        h, kept = x[0], []
        for n in range(layers):
            q, k, val = project(h, table, wq, wk, wv, n)
            o, lse = attend(q, k, val)
            kept.append((h, q, k, val, o, lse))
            if n < layers - 1:
                h = feed(h, o, wo, wg, wu, wd, n)
        dh = dy[0]
        TALL, WIDE = (6, 3), (0, 1, 2, 4, 5)
        moments = {TALL: None, WIDE: None}
        sums, blocks, wholes = {}, {}, []

        def stepped(which, n):
            fresh, moments[which] = update(me, sums[which, n], *([t[i] for i in which] for t in (weights, m, v)), n, moments[which])
            blocks.update(zip([(i, n) for i in which], fresh))

        for n in reversed(range(layers)):
            h, q, k, val, o, lse = kept[n]
            dmid, do, delta, g_tall, g_wide = feed_back(h, o, dh, wo, wg, wu, wd, n, devices)
            if n < layers - 1:
                g_tall, sums[WIDE, n + 1] = lax.optimization_barrier((g_tall, sums[WIDE, n + 1]))
            sums[TALL, n] = lax.psum_scatter(g_tall, "dp", scatter_dimension=0, tiled=True)
            dq, dk, dval = attend_back(q, k, val, do, lse, delta)
            g_wide, sums[TALL, n] = lax.optimization_barrier((g_wide, sums[TALL, n]))
            g_wide, dh = project_back(g_wide, h, table, dq, dk, dval, dmid if n else None, wq, wk, wv, n)
            sums[WIDE, n] = lax.psum_scatter(g_wide, "dp", scatter_dimension=0, tiled=True)
        for n in reversed(range(layers)):
            stepped(TALL, n)
            stepped(WIDE, n)
            wholes.append(gather([blocks[i, n] for i in range(7)], n))
        result = [None] * 21
        for i in range(7):
            result[i] = jnp.stack([whole[i] for whole in reversed(wholes)])
        for which in (TALL, WIDE):
            for at, i in enumerate(which):
                result[7 + i] = moments[which][at]
                result[14 + i] = moments[which][len(which) + at]
        return tuple(result)

    states, all_of, cut = P(("rep", "dp"), None, None), P(None, None, None), P(None, "dp", None)
    return jax.shard_map(
        step,
        mesh=mesh,
        in_specs=(states, states) + (all_of,) * 7 + (cut,) * 14,
        out_specs=(P("rep", None, None),) * 7 + (P("rep", "dp", None),) * 14,
        check_vma=False,
    )
```

```python
import numpy as np

import jax
import jax.numpy as jnp
from jax import lax
from jax.experimental import pallas as pl
from jax.experimental.pallas import tpu as pltpu
from jax.sharding import PartitionSpec as P

NEG = -1e30
LOG2E = 1.4426950408889634
HEAD = 128
THETA = 10000
BF, F32 = jnp.bfloat16, jnp.float32
ROWS = 512
PART = 512
ROOM = 60 * 2**20
MESH = pl.DeviceIdType.MESH


def _dot(a, b, ca, cb):
    return lax.dot_general(a, b, (((ca,), (cb,)), ((), ())), preferred_element_type=F32)


def _table(tokens):
    half = HEAD // 2
    angle = np.arange(tokens, dtype=np.float32)[:, None] * np.float32(THETA) ** (-np.arange(half, dtype=np.float32) / np.float32(half))
    return np.concatenate([np.cos(angle), np.sin(angle)], -1).astype(np.float32)


def _angles(tab):
    other = pltpu.roll(tab, HEAD // 2, 1)
    first = lax.broadcasted_iota(jnp.int32, tab.shape, 1) < HEAD // 2
    return jnp.where(first, tab, other), jnp.where(first, -other, tab)


def _normed(h):
    wide = h.astype(F32)
    scale = lax.rsqrt(jnp.mean(wide * wide, -1, keepdims=True) + 1e-6)
    return wide, scale, (wide * scale).astype(BF)


def _norm_back(wide, scale, d):
    dot = jnp.mean(d * wide, -1, keepdims=True)
    return scale * d - wide * (scale * scale * scale * dot)


def _heads(ref):
    return jnp.concatenate([ref[n] for n in range(ref.shape[0])], axis=1)


def _call(body, grid, given, ins, outs, out_specs, scratch=(), flops=0, aliases=None, prefetch=0):
    return pl.pallas_call(
        body,
        grid_spec=pltpu.PrefetchScalarGridSpec(num_scalar_prefetch=prefetch, grid=grid, in_specs=ins, out_specs=out_specs, scratch_shapes=list(scratch)),
        out_shape=outs,
        input_output_aliases=aliases or {},
        compiler_params=pltpu.CompilerParams(dimension_semantics=("arbitrary",) * len(grid), vmem_limit_bytes=ROOM),
        cost_estimate=pl.CostEstimate(flops=flops, transcendentals=0, bytes_accessed=sum(a.size * a.dtype.itemsize for a in [*given, *outs])),
    )(*given)


def _of(shape, dtype=BF):
    return jax.ShapeDtypeStruct(shape, dtype)


def _whole(shape, layer):
    return pl.BlockSpec((None, *shape[1:]), lambda i: (layer, 0, 0), pipeline_mode=pl.Buffered(1))


ROW = lambda d, rows=ROWS: pl.BlockSpec((rows, d), lambda i: (i, 0))
HROW = lambda heads, rows=ROWS: pl.BlockSpec((heads, rows, HEAD), lambda i: (0, i, 0))


def _seen():
    return lax.broadcasted_iota(jnp.int32, (ROWS, ROWS), 1) >= lax.broadcasted_iota(jnp.int32, (ROWS, ROWS), 0)


def _attention_call(body, given, ins, outs, out_specs, scratch, width):
    heads, tokens, _ = given[0].shape
    return _call(body, (tokens // ROWS,), given, ins, outs, out_specs, scratch, flops=heads * tokens * tokens * width)


WHOLE = lambda t: pl.BlockSpec(t.shape, lambda i, *_: (0, 0, 0))
STAT = lambda heads: pl.BlockSpec((heads, ROWS), lambda i, *_: (0, i))


def attend(q, k, v):
    heads, tokens, d = q.shape
    scale = d**-0.5
    e = scale * LOG2E

    def body(q_ref, k_ref, v_ref, o_ref, lse_ref, top_s, mix_s):
        iq = pl.program_id(0)
        top_s[...] = jnp.full(top_s.shape, NEG, F32)
        mix_s[...] = jnp.zeros_like(mix_s)
        ones = jnp.ones((8, ROWS), BF)

        def block(j, ok):
            here = pl.ds(j * ROWS, ROWS)
            scores = [_dot(k_ref[n, here, :], q_ref[n], 1, 1) for n in range(heads)]
            weights, keeps = [], []
            for n, s in enumerate(scores):
                if ok is not None:
                    s = jnp.where(ok, s, 2 * NEG)
                old = top_s[n : n + 1, :]
                top = jnp.maximum(old, s.max(axis=0, keepdims=True))
                top_s[n : n + 1, :] = top
                weights.append(jnp.exp2((s - top) * e).astype(BF))
                keeps.append(jnp.exp2((old - top) * e))
            for n, (p, keep) in enumerate(zip(weights, keeps)):
                values = jnp.concatenate([v_ref[n, here, :].T, ones], axis=0)
                mix_s[n] = mix_s[n] * keep + _dot(values, p, 1, 0)

        lax.fori_loop(0, iq, lambda j, _: block(j, None), None)
        block(iq, _seen())
        for n in range(heads):
            total = mix_s[n, d : d + 1, :]
            o_ref[n] = (mix_s[n, :d, :] * (1 / total)).T.astype(BF)
            lse_ref[n : n + 1, :] = top_s[n : n + 1, :] * scale + jnp.log(total)

    return _attention_call(body, [q, k, v], [HROW(heads), WHOLE(k), WHOLE(v)], [_of(q.shape), _of((heads, tokens), F32)],
                           [HROW(heads), STAT(heads)], [pltpu.VMEM((heads, ROWS), F32), pltpu.VMEM((heads, d + 8, ROWS), F32)], 2 * d)


def attend_back(q, k, v, do, lse, delta):
    heads, tokens, d = q.shape
    scale = d**-0.5
    e = scale * LOG2E

    def body(q_ref, k_ref, v_ref, do_ref, lse_ref, delta_ref, dq_ref, dk_ref, dv_ref, dq_s, dk_s, dv_s):
        iq = pl.program_id(0)

        @pl.when(iq == 0)
        def _():
            dk_s[...] = jnp.zeros_like(dk_s)
            dv_s[...] = jnp.zeros_like(dv_s)

        dq_s[...] = jnp.zeros_like(dq_s)

        def block(j, ok):
            here = pl.ds(j * ROWS, ROWS)
            scores = [_dot(k_ref[n, here, :], q_ref[n], 1, 1) for n in range(heads)]
            dps = [_dot(v_ref[n, here, :], do_ref[n], 1, 1) for n in range(heads)]
            for n in range(heads):
                p = jnp.exp2(scores[n] * e - lse_ref[n : n + 1, :] * LOG2E)
                if ok is not None:
                    p = jnp.where(ok, p, 0.0)
                ds = (p * (dps[n] - delta_ref[n : n + 1, :])).astype(BF)
                dv_s[n, here, :] += _dot(p.astype(BF), do_ref[n], 1, 0)
                dk_s[n, here, :] += _dot(ds, q_ref[n], 1, 0)
                dq_s[n] += _dot(k_ref[n, here, :].T, ds, 1, 0)

        lax.fori_loop(0, iq, lambda j, _: block(j, None), None)
        block(iq, _seen())
        for n in range(heads):
            dq_ref[n] = (dq_s[n] * scale).T.astype(BF)

        @pl.when(iq == pl.num_programs(0) - 1)
        def _():
            dk_ref[...] = (dk_s[...] * scale).astype(BF)
            dv_ref[...] = dv_s[...].astype(BF)

    return _attention_call(body, [q, k, v, do, lse, delta], [HROW(heads), WHOLE(k), WHOLE(v), HROW(heads), STAT(heads), STAT(heads)], [_of(q.shape)] * 3,
                           [HROW(heads), WHOLE(k), WHOLE(v)], [pltpu.VMEM((heads, d, ROWS), F32)] + [pltpu.VMEM(k.shape, F32)] * 2, 5 * d)


def project(h, table, wq, wk, wv, layer):
    tokens, d = h.shape
    heads = wq.shape[2] // HEAD

    def body(h_ref, tab_ref, wq_ref, wk_ref, wv_ref, q_ref, k_ref, v_ref):
        a = _normed(h_ref[...])[2]
        cos, sin = _angles(tab_ref[...])
        for w_ref, o_ref, turn in ((wq_ref, q_ref, True), (wk_ref, k_ref, True), (wv_ref, v_ref, False)):
            t = _dot(a, w_ref[...], 1, 0).astype(BF)
            for n in range(heads):
                x = t[:, n * HEAD : (n + 1) * HEAD]
                if turn:
                    x = x.astype(F32)
                    x = (x * cos + pltpu.roll(x, HEAD // 2, 1) * sin).astype(BF)
                o_ref[n] = x

    given = [h, table, wq, wk, wv]
    return _call(body, (tokens // ROWS,), given, [ROW(d), ROW(HEAD)] + [_whole(wq.shape, layer)] * 3, [_of((heads, tokens, HEAD))] * 3,
                 [HROW(heads)] * 3, flops=2 * tokens * d * d * 3)


def feed(h, o, wo, wg, wu, wd, layer):
    tokens, d = h.shape
    heads, ff = o.shape[0], wg.shape[2]

    def body(h_ref, o_ref, wo_ref, wg_ref, wu_ref, wd_ref, out_ref):
        mid = (h_ref[...].astype(F32) + _dot(_heads(o_ref), wo_ref[...], 1, 0).astype(BF).astype(F32)).astype(BF)
        b = _normed(mid)[2]
        down = jnp.zeros((ROWS, d), F32)
        for at in range(0, ff, PART):
            gate = _dot(b, wg_ref[:, at : at + PART], 1, 0)
            up = _dot(b, wu_ref[:, at : at + PART], 1, 0)
            act = (gate * lax.logistic(gate) * up).astype(BF)
            down += _dot(act, wd_ref[at : at + PART, :], 1, 0)
        out_ref[...] = (mid.astype(F32) + down.astype(BF).astype(F32)).astype(BF)

    given = [h, o, wo, wg, wu, wd]
    return _call(body, (tokens // ROWS,), given, [ROW(d), HROW(heads)] + [_whole(w.shape, layer) for w in (wo, wg, wu, wd)], [_of((tokens, d))],
                 [ROW(d)], flops=2 * tokens * d * (d + 3 * ff))[0]


def feed_back(h, o, dh, wo, wg, wu, wd, layer, devices):
    tokens, d = h.shape
    heads, ff = o.shape[0], wg.shape[2]
    tall_width, wide_width = ff + d, 3 * d + 2 * ff
    mine, tall = d // devices, ff // devices
    fold = tall // mine

    def body(h_ref, o_ref, dh_ref, wo_ref, wg_ref, wu_ref, wd_ref, dmid_ref, do_ref, delta_ref, tall_ref, wide_ref, ag, au, ad, ao):
        i = pl.program_id(0)

        @pl.when(i == 0)
        def _():
            for ref in (ag, au, ad, ao):
                ref[...] = jnp.zeros_like(ref)

        o = _heads(o_ref)
        mid = (h_ref[...].astype(F32) + _dot(o, wo_ref[...], 1, 0).astype(BF).astype(F32)).astype(BF)
        wide, scale, b = _normed(mid)
        dy = dh_ref[...]
        bt, dyt = b.T, dy.T
        db = jnp.zeros((ROWS, d), F32)
        for at in range(0, ff, PART):
            here = slice(at, at + PART)
            gate = _dot(b, wg_ref[:, here], 1, 0)
            up = _dot(b, wu_ref[:, here], 1, 0)
            da = _dot(dy, wd_ref[here, :], 1, 1).astype(BF).astype(F32)
            sig = lax.logistic(gate)
            silu = gate * sig
            act = (silu * up).astype(BF)
            dup = (da * silu).astype(BF)
            dgate = (da * up * (sig + silu * (1 - sig))).astype(BF)
            ad[:, here] += _dot(dyt, act, 1, 0)
            au[:, here] += _dot(bt, dup, 1, 0)
            ag[:, here] += _dot(bt, dgate, 1, 0)
            db += _dot(dgate, wg_ref[:, here], 1, 1) + _dot(dup, wu_ref[:, here], 1, 1)
        dmid = (dy.astype(F32) + _norm_back(wide, scale, db.astype(BF).astype(F32)).astype(BF).astype(F32)).astype(BF)
        dmid_ref[...] = dmid
        do = _dot(dmid, wo_ref[...], 1, 1).astype(BF)
        ao[...] += _dot(o.T, dmid, 1, 0)
        for n in range(heads):
            at = slice(n * HEAD, (n + 1) * HEAD)
            do_ref[n] = do[:, at]
            delta_ref[n : n + 1, :] = (do[:, at].astype(F32) * o[:, at].astype(F32)).T.sum(axis=0, keepdims=True)

        @pl.when(i == pl.num_programs(0) - 1)
        def _():
            wide_ref[:, 3 * d : 3 * d + ff] = ag[...].astype(BF)
            wide_ref[:, 3 * d + ff :] = au[...].astype(BF)
            tall_ref[:, ff:] = ao[...].astype(BF)
            for p in range(ff // HEAD):
                t = ad[:, p * HEAD : (p + 1) * HEAD].T.astype(BF)
                for q in range(HEAD // mine):
                    row = p * HEAD + q * mine
                    dev, j = row // tall, row % tall // mine
                    tall_ref[dev * mine : (dev + 1) * mine, j * d : (j + 1) * d] = t[q * mine : (q + 1) * mine, :]

    given = [h, o, dh, wo, wg, wu, wd]
    return _call(
        body, (tokens // ROWS,), given, [ROW(d), HROW(heads), ROW(d)] + [_whole(w.shape, layer) for w in (wo, wg, wu, wd)],
        [_of((tokens, d)), _of((heads, tokens, HEAD)), _of((heads, tokens), F32), _of((d, tall_width)), _of((d, wide_width))],
        [ROW(d), HROW(heads), pl.BlockSpec((heads, ROWS), lambda i: (0, i))]
        + [pl.BlockSpec((d, n), lambda i: (0, 0), pipeline_mode=pl.Buffered(1)) for n in (tall_width, wide_width)],
        [pltpu.VMEM((d, ff), F32)] * 3 + [pltpu.VMEM((d, d), F32)], flops=2 * tokens * d * (8 * ff + 3 * d))


def project_back(g, h, table, dq, dk, dv, dmid, wq, wk, wv, layer):
    tokens, d = h.shape
    heads = dq.shape[0]
    more = dmid is not None

    def body(_, h_ref, tab_ref, dq_ref, dk_ref, dv_ref, *rest):
        i = pl.program_id(0)
        ins, rest = (rest[:4], rest[4:]) if more else ((), rest)
        g_ref, acc = rest[0], rest[-1]
        wide, scale, a = _normed(h_ref[...])
        cos, sin = _angles(tab_ref[...])
        at = a.T

        @pl.when(i == 0)
        def _():
            acc[...] = jnp.zeros_like(acc)

        da = jnp.zeros((ROWS, d), F32)
        for n, (ref, turn) in enumerate(((dq_ref, True), (dk_ref, True), (dv_ref, False))):
            parts = []
            for m in range(heads):
                x = ref[m]
                if turn:
                    x = x.astype(F32)
                    x = (x * cos - pltpu.roll(x, HEAD // 2, 1) * sin).astype(BF)
                parts.append(x)
            t = jnp.concatenate(parts, axis=1)
            acc[:, n * d : (n + 1) * d] += _dot(at, t, 1, 0)
            if more:
                da += _dot(t, ins[1 + n][...], 1, 1)
        if more:
            dh = _norm_back(wide, scale, da.astype(BF).astype(F32)).astype(BF)
            rest[1][...] = (ins[0][...].astype(F32) + dh.astype(F32)).astype(BF)

        @pl.when(i == pl.num_programs(0) - 1)
        def _():
            g_ref[...] = acc[...].astype(BF)

    given = [g, h, table, dq, dk, dv] + ([dmid, wq, wk, wv] if more else [])
    got = _call(
        body, (tokens // ROWS,), given,
        [pl.BlockSpec(memory_space=pl.ANY), ROW(d), ROW(HEAD)] + [HROW(heads)] * 3 + ([ROW(d)] + [_whole(wq.shape, layer)] * 3 if more else []),
        [_of(g.shape)] + ([_of((tokens, d))] if more else []),
        [pl.BlockSpec((d, 3 * d), lambda i: (0, 0), pipeline_mode=pl.Buffered(1))] + ([ROW(d)] if more else []),
        [pltpu.VMEM((d, 3 * d), F32)], flops=2 * tokens * d * d * (6 if more else 3), aliases={0: 0})
    return got[0], got[1] if more else None


def update(me, g, w, m, v, layer, earlier):
    count = len(w)
    rows, width = g.shape
    steps = 4
    small = rows // steps
    folds = [one.shape[1] // rows for one in m]
    view = lambda t, f: t.reshape(t.shape[0], t.shape[1] // rows, rows, t.shape[2])
    given = [me, g] + [view(t, f) for t, f in zip(w, folds)] + [view(t, f) for t, f in zip(m, folds)] + [view(t, f) for t, f in zip(v, folds)]

    def body(me_ref, g_ref, *refs):
        ws, ms, vs = (refs[n * count : (n + 1) * count] for n in range(3))
        outs = refs[-3 * count :]
        at = 0
        for n in range(count):
            cols = ws[n].shape[2]
            for j in range(folds[n]):
                here = slice(at, at + cols)
                g = g_ref[:, here].astype(F32)
                new_m = 0.9 * ms[n][j] + 0.1 * g
                new_v = 0.95 * vs[n][j] + 0.05 * g * g
                old = ws[n][j].astype(F32)
                step = new_m * lax.rsqrt(new_v + 1e-8) + 0.1 * old
                outs[n][j] = (old - 0.02 * step).astype(BF)
                outs[count + n][j] = new_m
                outs[2 * count + n][j] = new_v
                at += cols

    moment = lambda t, f: pl.BlockSpec((None, f, small, t.shape[2]), lambda i, me_ref: (layer, 0, i, 0))
    weight = lambda t, f: pl.BlockSpec((None, f, small, t.shape[2]), lambda i, me_ref: (layer, me_ref[0], i, 0))
    moments = [moment(t, f) for t, f in zip(m, folds)] * 2
    wide = pl.BlockSpec((small, width), lambda i, me_ref: (i, 0))
    ins = [wide] + [weight(t, f) for t, f in zip(w, folds)] + moments
    aliases = {}
    if earlier is not None:
        aliases = {len(given) + n: count + n for n in range(2 * count)}
        given = given + [view(t, f) for t, f in zip(earlier, folds * 2)]
        ins = ins + [pl.BlockSpec(memory_space=pl.ANY)] * (2 * count)
    outs = [_of((f, rows, t.shape[2])) for t, f in zip(m, folds)] + [_of(view(t, f).shape, F32) for t, f in zip(m, folds)] * 2
    blocks = [pl.BlockSpec((f, small, t.shape[2]), lambda i, me_ref: (0, i, 0)) for t, f in zip(m, folds)]
    got = _call(body, (steps,), given, ins, outs, blocks + moments, flops=20 * rows * width, aliases=aliases, prefetch=1)
    return [t.reshape(f * rows, t.shape[2]) for t, f in zip(got, folds)], [t.reshape(o.shape) for t, o in zip(got[count:], [*m, *v])]


def gather(blocks, number):
    count, chips = len(blocks), 4

    def body(*refs):
        ins, outs, (up_s, up_r, down_s, down_r, twin_s, twin_r, own_s) = refs[:count], refs[count : 2 * count], refs[2 * count :]
        me = lax.axis_index("dp")
        z, core = me // 2, me % 2
        twin = me + 1 - 2 * core
        above, below = z < chips - 1, z > 0
        barrier = pltpu.get_barrier_semaphore()

        def greet(device):
            pl.semaphore_signal(barrier, inc=1, device_id={"dp": device}, device_id_type=MESH)

        greet(twin)
        pl.when(above)(lambda: greet(me + 2))
        pl.when(below)(lambda: greet(me - 2))
        pl.semaphore_wait(barrier, 1 + above.astype(jnp.int32) + below.astype(jnp.int32))

        def place(n, device):
            rows = ins[n].shape[0]
            return outs[n].at[pl.ds(pl.multiple_of(device * rows, rows), rows), :]

        def copy(n, src, device, sems, k, target):
            return pltpu.make_async_remote_copy(src_ref=src, dst_ref=place(n, device), send_sem=sems[0].at[n, k], recv_sem=sems[1].at[n, k],
                                                device_id={"dp": target}, device_id_type=MESH)

        UPS, DOWNS, TWINS = (up_s, up_r), (down_s, down_r), (twin_s, twin_r)
        each = range(count)
        mine = lambda n: pltpu.make_async_copy(ins[n], place(n, me), own_s.at[n])
        first = lambda n, sems, target: copy(n, ins[n], me, sems, 0, target)
        on = lambda n, device, sems, k, target: copy(n, place(n, device), device, sems, k, target)

        def all_of(what):
            def run():
                for n in each:
                    what(n)

            return run

        pl.when(above)(all_of(lambda n: first(n, UPS, me + 2).start()))
        pl.when(below)(all_of(lambda n: first(n, DOWNS, me - 2).start()))
        for n in each:
            first(n, TWINS, twin).start()
            mine(n).start()
        for t in range(1, chips):
            for near, far, sems, device, target, k in (
                (z >= t, above, UPS, me - 2 * t, me + 2, t), (z + t < chips, below, DOWNS, me + 2 * t, me - 2, chips - 1 + t)):

                @pl.when(near)
                def _():
                    for n in each:
                        on(n, device, sems, t - 1, twin).wait_recv()
                        if t < chips - 1:
                            pl.when(far)(lambda: on(n, device, sems, t, target).start())
                        on(n, device, TWINS, k, twin).start()

        for n in each:
            mine(n).wait()
            first(n, TWINS, twin).wait_send()
            on(n, twin, TWINS, 0, twin).wait_recv()
        pl.when(above)(all_of(lambda n: first(n, UPS, me + 2).wait_send()))
        pl.when(below)(all_of(lambda n: first(n, DOWNS, me - 2).wait_send()))
        for t in range(1, chips):
            for near, far, sems, device, target, k in (
                (z >= t, above, UPS, me - 2 * t, me + 2, t), (z + t < chips, below, DOWNS, me + 2 * t, me - 2, chips - 1 + t)):

                @pl.when(near)
                def _():
                    for n in each:
                        if t < chips - 1:
                            pl.when(far)(lambda: on(n, device, sems, t, target).wait_send())
                        on(n, device, TWINS, k, twin).wait_send()
                        on(n, device + 1 - 2 * core, TWINS, k, twin).wait_recv()

    hops = pltpu.SemaphoreType.DMA((count, chips - 1))
    return pl.pallas_call(
        body,
        in_specs=[pl.BlockSpec(memory_space=pltpu.VMEM)] * count,
        out_specs=[pl.BlockSpec(memory_space=pl.ANY)] * count,
        out_shape=[_of((8 * b.shape[0], b.shape[1])) for b in blocks],
        scratch_shapes=[hops] * 4 + [pltpu.SemaphoreType.DMA((count, 2 * chips - 1))] * 2 + [pltpu.SemaphoreType.DMA((count,))],
        compiler_params=pltpu.CompilerParams(collective_id=number, has_side_effects=True, vmem_limit_bytes=ROOM),
        cost_estimate=pl.CostEstimate(flops=10**10, transcendentals=0, bytes_accessed=10**7),
    )(*blocks)


def solution(mesh):
    devices = mesh.shape["dp"]

    def step(x, dy, *arrays):
        weights, m, v = (arrays[i : i + 7] for i in (0, 7, 14))
        wq, wk, wv, wo, wg, wu, wd = weights
        table = jnp.asarray(_table(x.shape[1]))
        layers = wq.shape[0]
        me = lax.axis_index("dp").astype(jnp.int32)[None]
        h, kept = x[0], []
        for n in range(layers):
            q, k, val = project(h, table, wq, wk, wv, n)
            o, lse = attend(q, k, val)
            kept.append((h, q, k, val, o, lse))
            if n < layers - 1:
                h = feed(h, o, wo, wg, wu, wd, n)
        dh = dy[0]
        TALL, WIDE = (6, 3), (0, 1, 2, 4, 5)
        moments = {TALL: None, WIDE: None}
        sums, blocks, wholes = {}, {}, []

        def stepped(which, n):
            fresh, moments[which] = update(me, sums[which, n], *([t[i] for i in which] for t in (weights, m, v)), n, moments[which])
            blocks.update(zip([(i, n) for i in which], fresh))

        def after(x, which, n):
            keys = [(i, n) for i in which]
            x, fresh = lax.optimization_barrier((x, [blocks[key] for key in keys]))
            blocks.update(zip(keys, fresh))
            return x

        for n in reversed(range(layers)):
            h, q, k, val, o, lse = kept[n]
            dmid, do, delta, g_tall, g_wide = feed_back(h, o, dh, wo, wg, wu, wd, n, devices)
            if n < layers - 1:
                stepped(TALL, n + 1)
                g_tall, sums[WIDE, n + 1] = lax.optimization_barrier((after(g_tall, TALL, n + 1), sums[WIDE, n + 1]))
            sums[TALL, n] = lax.psum_scatter(g_tall, "dp", scatter_dimension=0, tiled=True)
            dq, dk, dval = attend_back(q, k, val, do, lse, delta)
            if n < layers - 1:
                stepped(WIDE, n + 1)
                g_wide = after(g_wide, WIDE, n + 1)
            g_wide, sums[TALL, n] = lax.optimization_barrier((g_wide, sums[TALL, n]))
            g_wide, dh = project_back(g_wide, h, table, dq, dk, dval, dmid if n else None, wq, wk, wv, n)
            sums[WIDE, n] = lax.psum_scatter(g_wide, "dp", scatter_dimension=0, tiled=True)
        stepped(TALL, 0)
        blocks[0, layers - 1] = after(blocks[0, layers - 1], TALL, 0)
        for n in reversed(range(layers)):
            if n == 0:
                stepped(WIDE, n)
            wholes.append(gather([blocks[i, n] for i in range(7)], n))
        result = [None] * 21
        for i in range(7):
            result[i] = jnp.stack([whole[i] for whole in reversed(wholes)])
        for which in (TALL, WIDE):
            for at, i in enumerate(which):
                result[7 + i] = moments[which][at]
                result[14 + i] = moments[which][len(which) + at]
        return tuple(result)

    states, all_of, cut = P(("rep", "dp"), None, None), P(None, None, None), P(None, "dp", None)
    return jax.shard_map(
        step,
        mesh=mesh,
        in_specs=(states, states) + (all_of,) * 7 + (cut,) * 14,
        out_specs=(P("rep", None, None),) * 7 + (P("rep", "dp", None),) * 14,
        check_vma=False,
    )
```
